32 devices in a mesh: mod: 4 (over x, core), shard: 8 (over z, y).
Axes of the slice: x: 2, y: 2, z: 4, core: 2. Of those that a mesh axis runs over, the one named last changes fastest.
Arguments:
- tokens_b: bfloat16 [512, 4096], P(('mod', 'shard')), may hold values from -6 to 6
- labels_b: int32 [512, 1], P(('mod', 'shard')), may hold values from 0 to 3; in each aligned block of 16 rows (0 to 15, 16 to 31, ...) at most 6 rows name the same one
- tokens_a: bfloat16 [512, 4096], P(('mod', 'shard')), may hold values from -6 to 6
- labels_a: int32 [512, 1], P(('mod', 'shard')), may hold values from 0 to 3; in each aligned block of 16 rows (0 to 15, 16 to 31, ...) at most 6 rows name the same one
- grad_out_a: bfloat16 [512, 4096], P(('mod', 'shard')), may hold values from -6 to 6
- gate_saved: bfloat16 [4, 192, 11008], P('mod', None, 'shard'), may hold values from -6 to 6
- up_saved: bfloat16 [4, 192, 11008], P('mod', None, 'shard'), may hold values from -6 to 6
- gate_weight: bfloat16 [4, 4096, 11008], P('mod', None, 'shard'), may hold values from -0.09375 to 0.09375
- up_weight: bfloat16 [4, 4096, 11008], P('mod', None, 'shard'), may hold values from -0.09375 to 0.09375
- down_weight: bfloat16 [4, 11008, 4096], P('mod', 'shard'), may hold values from -0.0546875 to 0.0546875
Outputs:
- output_b: bfloat16 [512, 4096], P(('mod', 'shard'))
- grad_tokens_a: bfloat16 [512, 4096], P(('mod', 'shard'))
- grad_gate: bfloat16 [4, 4096, 11008], P('mod', None, 'shard')
- grad_up: bfloat16 [4, 4096, 11008], P('mod', None, 'shard')
- grad_down: bfloat16 [4, 11008, 4096], P('mod', 'shard')
The draws below stay inside these ranges and needn't reach their ends.
Inputs may be any that keep to these rules, and one draw needn't show every extreme that they name: `labels_b`: among the 16 tokens of one home device no label occurs more than 6 times; in every draw some home device has exactly 6 tokens of one label. `labels_a`: among the 16 tokens of one home device no label occurs more than 6 times; in every draw some home device has exactly 6 tokens of one label.
All inputs are finite; a program needn't handle non-finite values.
Results may differ from the reference program's by a relative error of at most 0.0049.
Values may be sent and summed in bfloat16 or wider, within the bound.
A program may use at most 128 MiB of HBM per device.

```python
import math
import jax
import jax.numpy as jnp
import numpy as np
from jax import lax

D = 4096
FF = 11008
MODS = 4
TOK_DEV = 16
CAP = 6
TOKENS = 512
ROWS = 192
N_MOD = 4
N_SHARD = 8


def level_of(rng, dims, pieces, smallest, top_value):
    level, own = 1.0, jax.random.fold_in(rng, 6)
    for dim, parts in pieces:
        heights = jnp.exp(jax.random.uniform(jax.random.fold_in(own, dim), (parts,), jnp.float32, smallest / len(pieces), top_value / len(pieces)))
        level = level * jnp.repeat(heights, dims[dim] // parts).reshape([-1 if axis == dim else 1 for axis in range(len(dims))])
    return level


def routed_block(own_key, own, number, rows, amount, top, reach, lean):
    order = jax.random.permutation(own_key, amount)
    crowded, ordinary = shares(amount, rows * top, reach, lean, True), shares(amount, rows * top, reach, lean, False)
    places = jnp.arange(amount)

    def named(tallies, rotation):
        used = int((tallies > 0).sum())
        fixed = max(1, used // 4)
        passed = fixed + (places - fixed + rotation * (used - fixed)) % max(1, amount - fixed)
        return jnp.zeros((amount,), jnp.int32).at[order[jnp.where(places < fixed, places, passed)]].set(jnp.asarray(tallies, jnp.int32))

    tallies = jnp.where(number % 4 == 0, named(crowded, number // 4), named(ordinary, number - number // 4 - 1))
    mixed = jax.random.permutation(jax.random.fold_in(own, 3), amount)
    source_of, receiver = mixed[0:amount // 2 * 2:2], mixed[1:amount // 2 * 2:2]
    margin = jnp.minimum(tallies[source_of] - 1, reach - tallies[receiver]) // 2
    margin = jnp.where((source_of == order[0]) | (receiver == order[0]) | (tallies[receiver] == 0), 0, jnp.maximum(margin, 0))
    passed = jax.random.randint(jax.random.fold_in(own, 4), (amount // 2,), 0, 1 << 20) % (margin + 1)
    tallies = tallies.at[source_of].add(-passed).at[receiver].add(passed)
    members = jnp.searchsorted(jnp.cumsum(tallies), jnp.arange(rows * top), side="right").astype(jnp.int32)
    listing = members.reshape(top, rows).T
    listing = listing[jax.random.permutation(jax.random.fold_in(own, 1), rows)]
    rotation = jax.random.randint(jax.random.fold_in(own, 2), (rows, 1), 0, top)
    return jnp.take_along_axis(listing, (jnp.arange(top)[None, :] + rotation) % top, axis=1)


def shares(number_of, total, limit, lean, full):
    portions = [(1 << 20) // math.isqrt(rank ** lean) + 1 for rank in range(1, number_of + 1)]
    largest = limit if full else min(limit, max(-(-total // number_of), total * portions[0] // sum(portions)))
    least = 1 if total - largest >= number_of - 1 else 0
    counts, spare = [largest] + [least] * (number_of - 1), total - largest - least * (number_of - 1)
    while spare > 0:
        movable = [i for i in range(1, number_of) if counts[i] < largest] or [i for i in range(1, number_of) if counts[i] < limit]
        whole, remaining = sum([portions[i] for i in movable]), spare
        for i in movable:
            more = min(limit - counts[i], max(1, remaining * portions[i] // whole), spare)
            counts[i] = counts[i] + more
            spare = spare - more
    return np.array(counts)


def centred(stream_key, extent, scale, most, split=(), held_as=jnp.bfloat16):
    result = scale * jax.random.normal(stream_key, extent, jnp.float32)
    if split:
        result = result * level_of(stream_key, extent, split, -0.22, 0.18)
    return jnp.clip(result, -most, most).astype(held_as)


def setup_inputs(seed: int = 0) -> dict:
    key_list = jax.random.split(jax.random.key(seed), 11)
    tokens_b = centred(key_list[0], (TOKENS, D), 1.0, 6.0, ((0, 32),))
    labels_b_keys = jax.random.split(jax.random.fold_in(key_list[1], 1), TOKENS // TOK_DEV)
    labels_b_turns = jax.random.permutation(jax.random.fold_in(key_list[1], 3), TOKENS // TOK_DEV)
    labels_b = jax.vmap(lambda own, number: routed_block(jax.random.fold_in(key_list[1], 2), own, number, TOK_DEV, N_MOD, 1, CAP, 2))(labels_b_keys, labels_b_turns).reshape((TOKENS, 1))
    tokens_a = centred(key_list[2], (TOKENS, D), 1.0, 6.0, ((0, 32),))
    labels_a_keys = jax.random.split(jax.random.fold_in(key_list[3], 1), TOKENS // TOK_DEV)
    labels_a_turns = jax.random.permutation(jax.random.fold_in(key_list[3], 3), TOKENS // TOK_DEV)
    labels_a = jax.vmap(lambda own, number: routed_block(jax.random.fold_in(key_list[3], 2), own, number, TOK_DEV, N_MOD, 1, CAP, 2))(labels_a_keys, labels_a_turns).reshape((TOKENS, 1))
    grad_out_a = centred(key_list[4], (TOKENS, D), 1.0, 6.0, ((0, 32),))
    gate_saved = centred(key_list[5], (MODS, ROWS, FF), 1.5, 6.0, ((0, 4), (2, 8)))
    up_saved = centred(key_list[6], (MODS, ROWS, FF), 1.0, 6.0, ((0, 4), (2, 8)))
    gate_weight = centred(key_list[7], (MODS, D, FF), D ** -0.5, 0.09375, ((0, 4), (2, 8)))
    up_weight = centred(key_list[8], (MODS, D, FF), D ** -0.5, 0.09375, ((0, 4), (2, 8)))
    down_weight = centred(key_list[9], (MODS, FF, D), FF ** -0.5, 0.0546875, ((0, 4), (1, 8)))
    return {"tokens_b": tokens_b, "labels_b": labels_b, "tokens_a": tokens_a, "labels_a": labels_a, "grad_out_a": grad_out_a, "gate_saved": gate_saved, "up_saved": up_saved, "gate_weight": gate_weight, "up_weight": up_weight, "down_weight": down_weight}


def place_table(labels):
    homes = N_MOD * N_SHARD
    lab = labels[:, 0].reshape(homes, TOK_DEV)
    onehot = (lab[:, :, None] == jnp.arange(N_MOD, dtype=jnp.int32)[None, None, :]).astype(jnp.int32)
    rank = jnp.cumsum(onehot, axis=1) - onehot
    slot = jnp.sum(rank * onehot, axis=2)
    within = (slot[:, :, None] == jnp.arange(CAP, dtype=jnp.int32)[None, None, :]).astype(jnp.int32)
    return (onehot[:, :, :, None] * within[:, :, None, :]).astype(jnp.float32)


def dispatch(place, values):
    homes = N_MOD * N_SHARD
    grid = jnp.einsum("htmc,htd->mhcd", place, values.reshape(homes, TOK_DEV, D).astype(jnp.float32))
    grid = grid.reshape(N_MOD, N_MOD, N_SHARD, CAP, D).transpose(0, 2, 1, 3, 4)
    return grid.reshape(N_MOD, ROWS, D).astype(jnp.bfloat16)


def collect(place, rows):
    homes = N_MOD * N_SHARD
    grid = rows.reshape(N_MOD, N_SHARD, N_MOD, CAP, D).transpose(0, 2, 1, 3, 4).reshape(N_MOD, homes, CAP, D)
    back = jnp.einsum("htmc,mhcd->htd", place, grid.astype(jnp.float32))
    return back.reshape(homes * TOK_DEV, D).astype(jnp.bfloat16)


def block_sum(pairs):
    width = FF // N_SHARD
    rows = pairs[0][0].shape[0]

    def step(total, index):
        part = jnp.zeros((rows, D), jnp.float32)
        for left, right in pairs:
            piece_left = lax.dynamic_slice_in_dim(left, index * width, width, 1)
            piece_right = lax.dynamic_slice_in_dim(right, index * width, width, 0)
            part = part + jnp.dot(piece_left, piece_right, preferred_element_type=jnp.float32)
        return total + part, None

    total, unused = lax.scan(step, jnp.zeros((rows, D), jnp.float32), jnp.arange(N_SHARD, dtype=jnp.int32))
    return total.astype(jnp.bfloat16)


def reference(tokens_b, labels_b, tokens_a, labels_a, grad_out_a, gate_saved, up_saved, gate_weight, up_weight, down_weight):
    place_b = place_table(labels_b)
    rows_b = dispatch(place_b, tokens_b)
    outputs = []
    for mode in range(N_MOD):
        gate = jnp.dot(rows_b[mode], gate_weight[mode], preferred_element_type=jnp.float32)
        up = jnp.dot(rows_b[mode], up_weight[mode], preferred_element_type=jnp.float32)
        hidden = (jax.nn.silu(gate) * up).astype(jnp.bfloat16)
        outputs.append(block_sum([(hidden, down_weight[mode])]))
    output_b = collect(place_b, jnp.stack(outputs))

    place_a = place_table(labels_a)
    rows_x = dispatch(place_a, tokens_a)
    rows_g = dispatch(place_a, grad_out_a)
    grads_x, grads_gate, grads_up, grads_down = [], [], [], []
    for mode in range(N_MOD):
        gate = gate_saved[mode].astype(jnp.float32)
        up = up_saved[mode].astype(jnp.float32)
        sig = jax.nn.sigmoid(gate)
        act = gate * sig
        dh = jnp.dot(rows_g[mode], down_weight[mode].T, preferred_element_type=jnp.float32)
        dgate = (dh * up * sig * (1.0 + gate * (1.0 - sig))).astype(jnp.bfloat16)
        dup = (dh * act).astype(jnp.bfloat16)
        hidden = (act * up).astype(jnp.bfloat16)
        grads_down.append(jnp.dot(hidden.T, rows_g[mode], preferred_element_type=jnp.float32).astype(jnp.bfloat16))
        grads_gate.append(jnp.dot(rows_x[mode].T, dgate, preferred_element_type=jnp.float32).astype(jnp.bfloat16))
        grads_up.append(jnp.dot(rows_x[mode].T, dup, preferred_element_type=jnp.float32).astype(jnp.bfloat16))
        grads_x.append(block_sum([(dgate, gate_weight[mode].T), (dup, up_weight[mode].T)]))
    grad_tokens_a = collect(place_a, jnp.stack(grads_x))
    return (output_b, grad_tokens_a, jnp.stack(grads_gate), jnp.stack(grads_up), jnp.stack(grads_down))
```

```python
import jax
import jax.numpy as jnp
from jax import lax
from jax.sharding import PartitionSpec as P

CAP = 6


def place_table(labels, modes):
    lab = labels[:, 0]
    onehot = (lab[:, None] == jnp.arange(modes, dtype=jnp.int32)[None, :]).astype(jnp.int32)
    rank = jnp.cumsum(onehot, axis=0) - onehot
    slot = jnp.sum(rank * onehot, axis=1)
    within = (slot[:, None] == jnp.arange(CAP, dtype=jnp.int32)[None, :]).astype(jnp.int32)
    table = onehot[:, :, None] * within[:, None, :]
    return table.reshape(lab.shape[0], modes * CAP).astype(jnp.bfloat16)


def dispatch(place, values, modes):
    sent = lax.dot_general(
        place, values, (((0,), (0,)), ((), ())), preferred_element_type=jnp.float32
    )
    return sent.astype(jnp.bfloat16).reshape(modes, CAP, values.shape[1])


def collect(place, arrived):
    flat = arrived.reshape(place.shape[1], arrived.shape[2])
    return jnp.dot(place, flat, preferred_element_type=jnp.float32).astype(jnp.bfloat16)


def contract_last(left, right):
    return lax.dot_general(
        left, right, (((1,), (1,)), ((), ())), preferred_element_type=jnp.float32
    )


def silu_mul(gate, up):
    return (jax.nn.silu(gate) * up).astype(jnp.bfloat16)


def body(
    tokens_b,
    labels_b,
    tokens_a,
    labels_a,
    grad_out_a,
    gate_saved,
    up_saved,
    gate_weight,
    up_weight,
    down_weight,
):
    gate_w, up_w, down_w = gate_weight[0], up_weight[0], down_weight[0]
    gate_s, up_s = gate_saved[0], up_saved[0]
    modes = lax.axis_size("mod")
    width = tokens_b.shape[1]
    rows = modes * CAP
    tie = lax.optimization_barrier

    place_a = place_table(labels_a, modes)
    place_b = place_table(labels_b, modes)

    def to_group(value):
        return lax.all_to_all(value, "mod", split_axis=0, concat_axis=0, tiled=True)

    def gather(value):
        return lax.all_gather(value, "shard", axis=0, tiled=True)

    arrived_g = to_group(dispatch(place_a, grad_out_a, modes))
    all_g = gather(arrived_g.reshape(rows, width))
    sent_rest = jnp.concatenate(
        [dispatch(place_b, tokens_b, modes), dispatch(place_a, tokens_a, modes)], axis=1
    )
    sent_rest, arrived_g = tie((sent_rest, arrived_g))
    arrived_rest = to_group(sent_rest)
    all_b = gather(arrived_rest[:, :CAP].reshape(rows, width))
    local_x = arrived_rest[:, CAP:].reshape(rows, width)

    gate = gate_s.astype(jnp.float32)
    up = up_s.astype(jnp.float32)
    sig = jax.nn.sigmoid(gate)
    act = gate * sig
    dh = contract_last(all_g, down_w)
    dgate = (dh * up * sig * (1.0 + gate * (1.0 - sig))).astype(jnp.bfloat16)
    dup = (dh * act).astype(jnp.bfloat16)
    hidden = (act * up).astype(jnp.bfloat16)
    terms_a = (contract_last(dgate, gate_w) + contract_last(dup, up_w)).astype(jnp.bfloat16)

    all_b, local_x, terms_a = tie((all_b, local_x, terms_a))
    summed_a = lax.psum_scatter(terms_a, "shard", scatter_dimension=0, tiled=True)
    all_x = gather(local_x)
    fwd_gate = jnp.dot(all_b, gate_w, preferred_element_type=jnp.float32)
    fwd_up = jnp.dot(all_b, up_w, preferred_element_type=jnp.float32)
    terms_b = jnp.dot(
        silu_mul(fwd_gate, fwd_up), down_w, preferred_element_type=jnp.float32
    ).astype(jnp.bfloat16)

    all_x, hidden, terms_b = tie((all_x, hidden, terms_b))
    summed_b = lax.psum_scatter(terms_b, "shard", scatter_dimension=0, tiled=True)
    outer = (((0,), (0,)), ((), ()))

    def weight_grad(left, right):
        return lax.dot_general(left, right, outer, preferred_element_type=jnp.float32).astype(
            jnp.bfloat16
        )

    grad_down = weight_grad(hidden, all_g)
    grad_gate = weight_grad(all_x, dgate)
    grad_up = weight_grad(all_x, dup)
    back_a = to_group(summed_a.reshape(modes, CAP, width))
    back_b = to_group(summed_b.reshape(modes, CAP, width))
    return (
        collect(place_b, back_b),
        collect(place_a, back_a),
        grad_gate[None],
        grad_up[None],
        grad_down[None],
    )


def solution(mesh):
    return jax.shard_map(
        body,
        mesh=mesh,
        in_specs=(
            P(("mod", "shard"), None),
            P(("mod", "shard"), None),
            P(("mod", "shard"), None),
            P(("mod", "shard"), None),
            P(("mod", "shard"), None),
            P("mod", None, "shard"),
            P("mod", None, "shard"),
            P("mod", None, "shard"),
            P("mod", None, "shard"),
            P("mod", "shard", None),
        ),
        out_specs=(
            P(("mod", "shard"), None),
            P(("mod", "shard"), None),
            P("mod", None, "shard"),
            P("mod", None, "shard"),
            P("mod", "shard", None),
        ),
        check_vma=False,
    )
```
